32 devices in a mesh: groups: 1, ep: 32 (over z, y, x, core).
Axes of the slice: x: 2, y: 2, z: 4, core: 2. Of those that a mesh axis runs over, the one named last changes fastest.
Arguments:
- tokens: bfloat16 [256, 7168], P(('groups', 'ep')), may hold values from -6 to 6
- expert_ids: int32 [256, 2], P(('groups', 'ep')), may hold values from 0 to 3, all different within a row; in each aligned block of 8 rows (0 to 7, 8 to 15, ...) at most 8 rows name the same one
- affinity: float32 [256, 2], P(('groups', 'ep')), may hold values from 0.05 to 1
- w_gate: bfloat16 [32, 7168, 256], P('ep'), may hold values from -0.0625 to 0.0625
- w_up: bfloat16 [32, 7168, 256], P('ep'), may hold values from -0.0625 to 0.0625
- w_down: bfloat16 [32, 256, 7168], P('ep'), may hold values from -0.125 to 0.125
Outputs:
- moe_out: bfloat16 [256, 7168], P(('groups', 'ep'))
The draws below stay inside these ranges and needn't reach their ends.
Inputs may be any that keep to these rules, and one draw needn't show every extreme that they name: `expert_ids`: each token names 2 different experts. Among the 8 tokens of one device no expert is named more than 8 times, and in every draw some device names some expert exactly 8 times.
All inputs are finite; a program needn't handle non-finite values.
Results may differ from the reference program's by a relative error of at most 0.008.
Values may be sent and summed in bfloat16 or wider, within the bound.
No kernel may reach another device: no remote copies, remote signals or barrier semaphores. Data moves between devices by JAX's collectives and lax.ppermute only.
A program may use at most 128 MiB of HBM per device.

```python
import math
import jax
import jax.numpy as jnp
import numpy as np
from jax import lax

D = 7168
FF = 2048
SPLIT = 8
ROUTES = 2
TOK_DEV = 8
HID_DEV = 256
EXPERTS = 4
PIECES = 32
CAP = 8
TOKENS = 256
N_EP = 32


def block_levels(rng, dims, cuts, smallest, top_value):
    level = 1.0
    for axis_at, parts in cuts:
        heights = jax.random.uniform(jax.random.fold_in(jax.random.fold_in(rng, 6), axis_at), (parts,), jnp.float32, smallest / len(cuts), top_value / len(cuts))
        level = level * jnp.repeat(jnp.exp(heights), dims[axis_at] // parts).reshape((-1,) + (1,) * (len(dims) - 1 - axis_at))
    return level


def assign_block(own_key, own, number, rows, count, top, most, skew):
    order = jax.random.permutation(own_key, count)
    heavy_load, usual = portions_of(count, rows * top, most, skew, True), portions_of(count, rows * top, most, skew, False)
    places = jnp.arange(count)

    def named(sizes, turn):
        used = int((sizes > 0).sum())
        fixed = max(1, used // 4)
        shifted = fixed + (places - fixed + turn * (used - fixed)) % max(1, count - fixed)
        return jnp.zeros((count,), jnp.int32).at[order[jnp.where(places < fixed, places, shifted)]].set(jnp.asarray(sizes, jnp.int32))

    sizes = jnp.where(number % 4 == 0, named(heavy_load, number // 4), named(usual, number - number // 4 - 1))
    mixed = jax.random.permutation(jax.random.fold_in(own, 3), count)
    donor, taker = mixed[0:count // 2 * 2:2], mixed[1:count // 2 * 2:2]
    margin = jnp.minimum(sizes[donor] - 1, most - sizes[taker]) // 2
    margin = jnp.where((donor == order[0]) | (taker == order[0]) | (sizes[taker] == 0), 0, jnp.maximum(margin, 0))
    shifted = jax.random.randint(jax.random.fold_in(own, 4), (count // 2,), 0, 1 << 20) % (margin + 1)
    sizes = sizes.at[donor].add(-shifted).at[taker].add(shifted)
    labels = jnp.searchsorted(jnp.cumsum(sizes), jnp.arange(rows * top), side="right").astype(jnp.int32)
    listing = labels.reshape(top, rows).T
    listing = listing[jax.random.permutation(jax.random.fold_in(own, 1), rows)]
    turn = jax.random.randint(jax.random.fold_in(own, 2), (rows, 1), 0, top)
    return jnp.take_along_axis(listing, (jnp.arange(top)[None, :] + turn) % top, axis=1)


def portions_of(number_of, total, limit, lean, full):
    portions = [(1 << 20) // math.isqrt(standing ** lean) + 1 for standing in range(1, number_of + 1)]
    largest = limit if full else min(limit, max(-(-total // number_of), total * portions[0] // sum(portions)))
    least = 1 if total - largest >= number_of - 1 else 0
    given, spare = [largest] + [least] * (number_of - 1), total - largest - least * (number_of - 1)
    while spare > 0:
        candidates = [i for i in range(1, number_of) if given[i] < largest] or [i for i in range(1, number_of) if given[i] < limit]
        whole, budget = sum([portions[i] for i in candidates]), spare
        for i in candidates:
            more = min(limit - given[i], max(1, budget * portions[i] // whole), spare)
            given[i] = given[i] + more
            spare = spare - more
    return np.array(given)


def scatter_about(stream_key, shape, width, bound, shards=(), kind=jnp.bfloat16):
    factor_of = block_levels(stream_key, shape, shards, -0.22, 0.18) if shards else 1.0
    drawn = jax.random.normal(stream_key, shape, jnp.float32) * width * factor_of
    return jnp.minimum(jnp.maximum(drawn, -bound), bound).astype(kind)


def setup_inputs(seed: int = 0, part: int = 0) -> dict:
    keys = jax.random.split(jax.random.key(seed), 7)
    part_keys = jax.random.split(jax.random.fold_in(keys[6], part), 7)
    tokens = scatter_about(part_keys[0], (TOKENS, D), 1.0, 6.0, ((0, 32),))
    expert_ids_keys = jax.random.split(jax.random.fold_in(part_keys[1], 1), TOKENS // TOK_DEV)
    expert_ids_turns = jax.random.permutation(jax.random.fold_in(part_keys[1], 3), TOKENS // TOK_DEV)
    expert_ids = jax.vmap(lambda own, number: assign_block(jax.random.fold_in(part_keys[1], 2), own, number, TOK_DEV, EXPERTS, ROUTES, CAP, 2))(expert_ids_keys, expert_ids_turns).reshape((TOKENS, ROUTES))
    affinity = jnp.clip(jnp.exp(math.log(1.0) - 2.9957323 * jax.random.uniform(part_keys[2], (TOKENS, ROUTES), jnp.float32) ** block_levels(part_keys[2], (TOKENS, ROUTES), ((0, 32),), -0.2, 0.2)), 0.05, 1.0)
    w_gate = scatter_about(keys[3], (PIECES, D, HID_DEV), D ** -0.5, 0.0625, ((0, 32),))
    w_up = scatter_about(keys[4], (PIECES, D, HID_DEV), D ** -0.5, 0.0625, ((0, 32),))
    w_down = scatter_about(keys[5], (PIECES, HID_DEV, D), FF ** -0.5, 0.125, ((0, 32),))
    return {"tokens": tokens, "expert_ids": expert_ids, "affinity": affinity, "w_gate": w_gate, "w_up": w_up, "w_down": w_down}


route_scale = 2.5


def reference(tokens, expert_ids, affinity, w_gate, w_up, w_down):
    route_weight = route_scale * affinity / jnp.sum(affinity, axis=1, keepdims=True)
    onehot = (expert_ids.reshape(N_EP, TOK_DEV * ROUTES, 1) == jnp.arange(EXPERTS, dtype=jnp.int32)[None, None, :]).astype(jnp.int32)
    earlier = jnp.cumsum(onehot, axis=1) - onehot
    slot = jnp.sum(earlier * onehot, axis=2).reshape(TOKENS, ROUTES).astype(jnp.int32)
    source = (jnp.arange(TOKENS, dtype=jnp.int32) // TOK_DEV)[:, None]
    position = (source * CAP + slot).astype(jnp.int32)
    token_index = jnp.broadcast_to(jnp.arange(TOKENS, dtype=jnp.int32)[:, None], (TOKENS, ROUTES))
    table = jnp.full((EXPERTS, N_EP * CAP), TOKENS, jnp.int32).at[expert_ids, position].set(token_index)
    padded = jnp.concatenate([tokens, jnp.zeros((1, D), jnp.bfloat16)], axis=0)

    def expert_rows(expert):
        rows = padded[table[expert]]
        total = jnp.zeros((N_EP * CAP, D), jnp.float32)
        for piece_slot in range(SPLIT):
            piece = (expert * SPLIT + piece_slot).astype(jnp.int32)
            gate_piece = lax.dynamic_index_in_dim(w_gate, piece, 0, keepdims=False)
            up_piece = lax.dynamic_index_in_dim(w_up, piece, 0, keepdims=False)
            down_piece = lax.dynamic_index_in_dim(w_down, piece, 0, keepdims=False)
            gate = jnp.dot(rows, gate_piece, preferred_element_type=jnp.float32)
            up = jnp.dot(rows, up_piece, preferred_element_type=jnp.float32)
            hidden = (jax.nn.silu(gate) * up).astype(jnp.bfloat16)
            partial_value = jnp.dot(hidden, down_piece, preferred_element_type=jnp.float32).astype(jnp.bfloat16)
            total = total + partial_value.astype(jnp.float32)
        return total

    outputs = lax.map(expert_rows, jnp.arange(EXPERTS, dtype=jnp.int32))
    picked = outputs[expert_ids, position]
    return jnp.sum(route_weight[:, :, None] * picked, axis=1).astype(jnp.bfloat16)
```

```python
import jax
import jax.numpy as jnp
from jax import lax
from jax.sharding import PartitionSpec as P

SPLIT = 8
CHUNKS = 2


route_scale = 2.5


def slots_of(expert_ids, experts):
    flat = expert_ids.reshape(-1)
    onehot = (flat[:, None] == jnp.arange(experts, dtype=jnp.int32)[None, :]).astype(jnp.int32)
    earlier = jnp.cumsum(onehot, axis=0) - onehot
    return jnp.sum(earlier * onehot, axis=1).reshape(expert_ids.shape)


def body(tokens, expert_ids, affinity, w_gate, w_up, w_down):
    devices = lax.axis_size("ep")
    experts = devices // SPLIT
    tok_rows, width = tokens.shape
    routes = expert_ids.shape[1]
    capacity = min(tok_rows, max(2, 2 * tok_rows * routes // experts))
    packed = capacity < tok_rows

    def rotate(value, planes):
        pairs = [(i, (i + planes * SPLIT) % devices) for i in range(devices)]
        return lax.ppermute(value, "ep", pairs)

    def swap(value, bit):
        return lax.ppermute(value, "ep", [(i, i ^ bit) for i in range(devices)])

    cat = lambda parts: parts[0] if len(parts) == 1 else jnp.concatenate(parts, axis=0)

    route_weight = route_scale * affinity / jnp.sum(affinity, axis=1, keepdims=True)
    own_expert = lax.axis_index("ep") // SPLIT
    if packed:
        slot = slots_of(expert_ids, experts)

    def choose(k):
        expert = (own_expert + k) % experts
        named = expert_ids == expert
        if not packed:
            return None, jnp.sum(jnp.where(named, route_weight, 0.0), axis=1, keepdims=True)
        hit = (slot[:, :, None] == jnp.arange(capacity, dtype=jnp.int32)) & named[:, :, None]
        return (
            jnp.sum(hit.astype(jnp.float32), axis=1),
            jnp.sum(jnp.where(hit, route_weight[:, :, None], 0.0), axis=1),
        )

    selects = [choose(k) for k in range(experts)]

    def rows_for(k):
        if not packed:
            return tokens
        select = selects[k][0].astype(jnp.bfloat16)
        return jnp.dot(select.T, tokens, preferred_element_type=jnp.float32).astype(jnp.bfloat16)

    groups = [rows_for(0)] + [rotate(rows_for(k), k) for k in range(1, experts)]
    per_chunk = experts // CHUNKS

    def spread(first, second, bits):
        near = swap(first, bits[0])
        far = swap(cat([first, near]), bits[1])
        return cat([first, near, far])

    def collect(blocks, bits):
        half = blocks.shape[0] // 2
        kept = add(blocks[:half], swap(blocks[half:], bits[1]))
        half //= 2
        return add(kept[:half], swap(kept[half:], bits[0]))

    def add(a, b):
        return (a.astype(jnp.float32) + b.astype(jnp.float32)).astype(jnp.bfloat16)

    def expert(rows):
        gate = jnp.dot(rows, w_gate[0], preferred_element_type=jnp.float32)
        up = jnp.dot(rows, w_up[0], preferred_element_type=jnp.float32)
        hidden = (jax.nn.silu(gate) * up).astype(jnp.bfloat16)
        return jnp.dot(hidden, w_down[0], preferred_element_type=jnp.float32)

    backs = []
    for chunk in range(CHUNKS):
        mine = range(chunk * per_chunk, (chunk + 1) * per_chunk)
        colours = [(list(mine[0::2]), (2, 4)), (list(mine[1::2]), (4, 2))]
        colours = [(members, bits) for members, bits in colours if members]
        here = cat([spread(cat([groups[g] for g in members]), None, bits) for members, bits in colours])
        size = here.shape[0]
        rows = cat([here, swap(here, 1)])
        partial_value = expert(rows).astype(jnp.bfloat16)
        chip = add(partial_value[:size], swap(partial_value[size:], 1))
        at = 0
        for members, bits in colours:
            count = 4 * len(members) * capacity
            got = collect(chip[at : at + count], bits)
            at += count
            for i, g in enumerate(members):
                backs.append((g, got[i * capacity : (i + 1) * capacity]))

    mixed = jnp.zeros((tok_rows, width), jnp.float32)
    for g, value in backs:
        home = (value if g == 0 else rotate(value, -g)).astype(jnp.float32)
        if packed:
            mixed = mixed + jnp.dot(
                selects[g][1], home, precision=lax.Precision.HIGHEST, preferred_element_type=jnp.float32
            )
        else:
            mixed = mixed + selects[g][1] * home
    return mixed.astype(jnp.bfloat16)


def solution(mesh):
    return jax.shard_map(
        body,
        mesh=mesh,
        in_specs=(
            P(("groups", "ep"), None),
            P(("groups", "ep"), None),
            P(("groups", "ep"), None),
            P("ep", None, None),
            P("ep", None, None),
            P("ep", None, None),
        ),
        out_specs=P(("groups", "ep"), None),
        check_vma=False,
    )
```
